8 devices in a mesh: batch: 1 (over z), z: 2 (over y), y: 2 (over x), x: 2 (over core).
Axes of the slice: x: 2, y: 2, z: 1, core: 2. Of those that a mesh axis runs over, the one named last changes fastest.
Arguments:
- volume: bfloat16 [64, 128, 128, 128], P('batch', 'x', 'y', 'z')
- filter_taps: float32 [3, 3, 21], replicated
- mix_w: bfloat16 [3, 64, 64], replicated
- mix_bias: float32 [3, 64], replicated
Outputs:
- output: bfloat16 [64, 128, 128, 128], P('batch', 'x', 'y', 'z')
All inputs are finite; a program needn't handle non-finite values.
Results may differ from the reference program's by a relative error of at most 0.00616.
Values are sent between devices in bfloat16 or wider.
A program may use at most 1 GiB of HBM per device.

```python
import jax
import jax.numpy as jnp
from jax import lax

CHANNELS = 64
KERNEL = 21
LAYERS = 3
GRID_X = 128
GRID_Y = 128
GRID_Z = 128
HALF = (KERNEL - 1) // 2


def setup_inputs(seed: int = 0, part: int = 0) -> dict:
    vol_key = jax.random.fold_in(jax.random.key(seed), part)
    key_mag, key_sign, key_mix, key_bias = jax.random.split(jax.random.key(seed + 1), 4)
    volume = jax.random.normal(vol_key, (CHANNELS, GRID_X, GRID_Y, GRID_Z), jnp.float32)
    tap_mag = jax.random.uniform(key_mag, (LAYERS, 3, KERNEL), jnp.float32, 0.5, 1.5)
    tap_sign = jax.random.bernoulli(key_sign, 0.5, (LAYERS, 3, KERNEL)).astype(jnp.float32) * 2.0 - 1.0
    filter_taps = tap_sign * tap_mag * (KERNEL ** -0.5)
    mix_w = jax.random.normal(key_mix, (LAYERS, CHANNELS, CHANNELS), jnp.float32) * (CHANNELS ** -0.5)
    mix_bias = 0.5 * jax.random.normal(key_bias, (LAYERS, CHANNELS), jnp.float32)
    return {"volume": volume.astype(jnp.bfloat16), "filter_taps": filter_taps, "mix_w": mix_w.astype(jnp.bfloat16), "mix_bias": mix_bias}


def axis_pass(chan_vol, taps_row, axis_pos):
    pad_widths = tuple((HALF, HALF) if dim_idx == axis_pos else (0, 0) for dim_idx in range(3))
    padded = jnp.pad(chan_vol.astype(jnp.float32), pad_widths)
    length = chan_vol.shape[axis_pos]
    accum_sum = jnp.zeros(chan_vol.shape, jnp.float32)
    for offset in range(KERNEL):
        accum_sum = accum_sum + taps_row[offset] * lax.slice_in_dim(padded, offset, offset + length, axis=axis_pos)
    return accum_sum.astype(jnp.bfloat16)


def reference(volume, filter_taps, mix_w, mix_bias):
    taps_b = filter_taps.astype(jnp.bfloat16).astype(jnp.float32)

    def layer_step(carry_vol, layer_in):
        layer_taps, layer_w, layer_b = layer_in

        def channel_filter(chan_vol):
            staged = axis_pass(chan_vol, layer_taps[0], 0)
            staged = axis_pass(staged, layer_taps[1], 1)
            return axis_pass(staged, layer_taps[2], 2)

        filtered = lax.map(channel_filter, carry_vol)
        mixed_out = jnp.dot(layer_w.T, filtered.reshape(CHANNELS, -1), preferred_element_type=jnp.float32)
        activated = jax.nn.gelu(mixed_out + layer_b[:, None], approximate=False)
        new_vol = (carry_vol.astype(jnp.float32) + activated.reshape(carry_vol.shape)).astype(jnp.bfloat16)
        return new_vol, None

    final_vol, _ = lax.scan(layer_step, volume, (taps_b, mix_w, mix_bias))
    return final_vol
```

```python
import functools

import jax
import jax.numpy as jnp
from jax import lax
from jax.experimental import pallas as pl
from jax.experimental.pallas import tpu as pltpu
from jax.sharding import PartitionSpec as P


CI = 16
NT = (((1,), (1,)), ((), ()))
KB = 16
XQ = 4
YI = 4
YQ = 4
ZQ = 4
LJ = 16
LQ = 4
EJ = 16
EQ = 4
PAD = 1
LANES = 128
F32 = jnp.float32
BF16 = jnp.bfloat16


def toeplitz(taps, offset):
    half = (taps.shape[1] - 1) // 2
    hits = (offset + half)[None, ..., None] == jnp.arange(taps.shape[1])
    taps_b = taps.astype(BF16).astype(F32)
    return jnp.sum(jnp.where(hits, taps_b[:, None, None, :], 0.0), axis=-1).astype(BF16)


def band_x(taps, x_pos):
    n = jnp.arange(2 * CI)[:, None]
    q = jnp.arange(4 * CI)[None, :]
    sign = jnp.where(x_pos == 0, 1, -1)
    return toeplitz(taps, sign * CI * (q // CI - 1 - n // CI) + q % CI - n % CI)


FAR = 10**6


def band_y(taps, y_pos, jl_len):
    half = (taps.shape[1] - 1) // 2
    n = jnp.arange(jl_len)[:, None]
    m = jnp.arange(jl_len)
    r = jnp.arange(16)
    other = jnp.where(m < jl_len // 2, m + jl_len, m - jl_len)
    beyond = jnp.where(r < half, jnp.where(y_pos == 0, jl_len + r, r - half), FAR)
    return toeplitz(taps, jnp.concatenate([m, other, beyond])[None, :] - n)


def band_z(taps, z_pos, k_len):
    half = (taps.shape[1] - 1) // 2
    n = jnp.arange(k_len)[:, None]
    r = jnp.arange(16)
    beyond = jnp.where(r < half, jnp.where(z_pos == 0, k_len + r, r - half), FAR)
    return toeplitz(taps, jnp.concatenate([jnp.arange(k_len), beyond])[None, :] - n)


def lane_low(shape):
    return lax.broadcasted_iota(jnp.int32, shape, 1) < LANES // 2


def swap_halves(v):
    return pltpu.roll(v, LANES // 2, 1)


def x_kernel(n_in, half, meta, a_ref, *refs):
    vols, u_ref, sends, s_ref = refs[:n_in], refs[n_in], refs[n_in + 1 : -1], refs[-1]
    jl_len, ci = vols[0].shape[0], vols[0].shape[2]
    planes = len(sends) * ci
    row = planes + PAD
    y_pos = meta[1]
    first = jnp.where(y_pos == 0, jl_len - half, 0)
    group = 8
    mat = a_ref[0]

    def pair(kp, slot):
        for par in range(2):
            k = kp * 2 + par
            for g in range(0, jl_len, group):
                rhs = jnp.concatenate(
                    [jnp.concatenate([v[jl, k] for v in vols], axis=0) for jl in range(g, g + group)], axis=1
                )
                out = jnp.dot(mat, rhs, preferred_element_type=F32)
                for t in range(group):
                    s_ref[slot + par, pl.ds((g + t) * row, planes), :] = out[:, t * LANES : (t + 1) * LANES]

    def finish(kp, slot):
        for par in range(2):
            for i in range(planes):
                u_ref[i, kp * 2 + par] = s_ref[slot + par, pl.ds(i, jl_len, stride=row), :].astype(BF16)
        for r in range(half):
            for part, send_ref in enumerate(sends):
                rows = pl.ds((first + r) * row + part * ci, ci)
                even, odd = s_ref[slot, rows, :], s_ref[slot + 1, rows, :]
                low = lane_low(even.shape)
                up = jnp.where(low, swap_halves(even), odd)
                down = jnp.where(low, even, swap_halves(odd))
                send_ref[kp, r] = jnp.where(y_pos == 0, up, down).astype(BF16)

    def body(step, _):
        for q in range(XQ):
            pair(step * XQ + q, 2 * q)
            if q:
                finish(step * XQ + q - 1, 2 * (q - 1))
        finish(step * XQ + XQ - 1, 2 * (XQ - 1))
        return 0

    lax.fori_loop(0, vols[0].shape[1] // (2 * XQ), body, 0)


def x_pass(meta, mats, layer, vols, half):
    jl_len, k_len, ci, _ = vols[0].shape
    n_in, n_own = len(vols), mats.shape[1] // CI
    vol_spec = pl.BlockSpec((jl_len, KB, ci, LANES), lambda s, m: (0, s, 0, 0))
    send_spec = pl.BlockSpec((KB // 2, half, ci, LANES), lambda s, m: (s, 0, 0, 0))
    send_shape = jax.ShapeDtypeStruct((k_len // 2, half, ci, LANES), BF16)
    size = jl_len * k_len * ci * LANES
    return pl.pallas_call(
        functools.partial(x_kernel, n_in, half),
        grid_spec=pltpu.PrefetchScalarGridSpec(
            num_scalar_prefetch=1,
            grid=(k_len // KB,),
            in_specs=[pl.BlockSpec((1, *mats.shape[1:]), lambda s, m: (layer, 0, 0))] + [vol_spec] * n_in,
            out_specs=[pl.BlockSpec((n_own * ci, KB, jl_len, LANES), lambda s, m: (0, s, 0, 0))] + [send_spec] * n_own,
            scratch_shapes=[pltpu.VMEM((2 * XQ, jl_len * (n_own * ci + PAD), LANES), F32)],
        ),
        out_shape=[jax.ShapeDtypeStruct((n_own * ci, k_len, jl_len, LANES), BF16)] + [send_shape] * n_own,
        cost_estimate=pl.CostEstimate(flops=size * 512 * n_own, bytes_accessed=size * 2 * (n_in + n_own), transcendentals=0),
        name="x_pass",
    )(meta, mats, *vols)


def y_kernel(half, meta, a_ref, u_ref, nb_ref, o_ref, send_ref, nb_s, s_ref):
    y_pos, z_pos = meta[1], meta[2]
    k_len, jl_len = u_ref.shape[1], u_ref.shape[2]
    ci = nb_ref.shape[2]
    mat = a_ref[0]
    pitch = ci + PAD
    span = 16 * pitch
    row = jl_len + PAD

    @pl.when(pl.program_id(0) == 0)
    def _():
        def fill(kp, _):
            for r in range(16):
                rows = pl.ds(kp * span + r * pitch, ci)
                nb_s[rows, :] = nb_ref[kp, r].astype(F32) if r < half else jnp.zeros((ci, LANES), F32)
            return 0

        lax.fori_loop(0, k_len // 2, fill, 0)

    first = jnp.where(z_pos == 0, k_len - half, 0)

    def quad(here_i, slot, kq):
        i = pl.program_id(0) * YI + here_i
        parts = []
        for pr in range(2):
            kp = kq * 2 + pr
            nb = nb_s[pl.ds(kp * span + i, 16, stride=pitch), :]
            turned = swap_halves(nb)
            here = lane_low(nb.shape) == (y_pos != 0)
            for par in range(2):
                k = kp * 2 + par
                own = u_ref[here_i, k]
                other = swap_halves(own.astype(F32))
                top = lax.broadcasted_iota(jnp.int32, other.shape, 0) < jl_len // 2
                other = jnp.where(top == lane_low(other.shape), other, 0.0).astype(BF16)
                stay = (y_pos == 0) if par else (y_pos != 0)
                far = jnp.where(here, jnp.where(stay, nb, turned), 0.0).astype(BF16)
                parts.append(jnp.concatenate([own, other, far], axis=0))
        out = jnp.dot(mat, jnp.concatenate(parts, axis=1), preferred_element_type=F32)
        for t in range(4):
            rows = pl.ds((kq * 4 + t) * row, jl_len)
            s_ref[slot, rows, :] = out[:, t * LANES : (t + 1) * LANES]

    def finish(here_i, slot):
        for jl in range(jl_len):
            o_ref[here_i, jl] = s_ref[slot, pl.ds(jl, k_len, stride=row), :].astype(BF16)
        for r in range(half):
            for jb in range(jl_len // 8):
                rows = pl.ds((first + r) * row + jb * 8, 8)
                send_ref[here_i, jb, r] = s_ref[slot, rows, :].astype(BF16)

    def body(step, _):
        for q in range(YQ):
            for kq in range(k_len // 4):
                quad(step * YQ + q, q, kq)
            if q:
                finish(step * YQ + q - 1, q - 1)
        finish(step * YQ + YQ - 1, YQ - 1)
        return 0

    lax.fori_loop(0, YI // YQ, body, 0)


def y_pass(meta, mats, layer, u1, part, nb, half):

    ci, k_len, jl_len = nb.shape[2], u1.shape[1], u1.shape[2]
    size = jl_len * k_len * ci * LANES
    return pl.pallas_call(
        functools.partial(y_kernel, half),
        grid_spec=pltpu.PrefetchScalarGridSpec(
            num_scalar_prefetch=1,
            grid=(ci // YI,),
            in_specs=[
                pl.BlockSpec((1, *mats.shape[1:]), lambda s, m: (layer, 0, 0)),
                pl.BlockSpec((YI, k_len, jl_len, LANES), lambda s, m: (s + part * (ci // YI), 0, 0, 0)),
                pl.BlockSpec(nb.shape, lambda s, m: (0, 0, 0, 0)),
            ],
            out_specs=[
                pl.BlockSpec((YI, jl_len, k_len, LANES), lambda s, m: (s, 0, 0, 0)),
                pl.BlockSpec((YI, jl_len // 8, half, 8, LANES), lambda s, m: (s, 0, 0, 0, 0)),
            ],
            scratch_shapes=[
                pltpu.VMEM((k_len // 2 * 16 * (ci + PAD), LANES), F32),
                pltpu.VMEM((YQ, k_len * (jl_len + PAD), LANES), F32),
            ],
        ),
        out_shape=[
            jax.ShapeDtypeStruct((ci, jl_len, k_len, LANES), BF16),
            jax.ShapeDtypeStruct((ci, jl_len // 8, half, 8, LANES), BF16),
        ],
        cost_estimate=pl.CostEstimate(flops=size * 160 * 4, bytes_accessed=size * 5, transcendentals=0),
        name="y_pass",
    )(meta, mats, u1, nb)


class Mixer:
    def __init__(self, half, a_ref, w_ref, b_ref, u_ref, nb_ref, nb_s, u3_s):
        self.ci, self.jb, self.k_len = u_ref.shape[0], u_ref.shape[1], u_ref.shape[2]
        self.half, self.a_ref, self.w_ref, self.b_ref = half, a_ref, w_ref, b_ref
        self.u_ref, self.nb_ref, self.nb_s, self.u3_s = u_ref, nb_ref, nb_s, u3_s
        self.pitch = self.jb + PAD
        self.span = 16 * self.pitch

    def fill(self):
        def one(i, _):
            for r in range(16):
                rows = pl.ds(i * self.span + r * self.pitch, self.jb)
                far = self.nb_ref[i, 0, r].astype(F32) if r < self.half else jnp.zeros((self.jb, LANES), F32)
                self.nb_s[rows, :] = far
            return 0

        lax.fori_loop(0, self.ci, one, 0)

    def filt(self, jl, slot):
        for ip in range(self.ci // 2):
            parts = []
            for i in (2 * ip, 2 * ip + 1):
                far = self.nb_s[pl.ds(i * self.span + jl, 16, stride=self.pitch), :].astype(BF16)
                parts.append(jnp.concatenate([self.u_ref[i, jl], far], axis=0))
            u3 = jnp.dot(self.a_ref[0], jnp.concatenate(parts, axis=1), preferred_element_type=F32)
            self.u3_s[slot, pl.ds(ip * self.k_len, self.k_len), :] = u3.astype(BF16)

    def gelu(self, ip, slot):
        u3 = self.u3_s[slot, pl.ds(ip * self.k_len, self.k_len), :]
        m = jnp.dot(u3, self.w_ref[0], preferred_element_type=F32) + self.b_ref[0]
        return 0.5 * m * (1.0 + lax.erf(m * 0.7071067811865476))


def z_kernel(half, a_ref, w_ref, b_ref, u_ref, nb_ref, v_ref, o_ref, nb_s, u3_s, g_s):
    mixer = Mixer(half, a_ref, w_ref, b_ref, u_ref, nb_ref, nb_s, u3_s)
    ci, k_len = mixer.ci, mixer.k_len
    row = k_len + PAD
    mixer.fill()

    def mix(slot):
        for ip in range(ci // 2):
            g = mixer.gelu(ip, slot)
            for t in range(2):
                g_s[slot, pl.ds((2 * ip + t) * row, k_len), :] = g[:, t * LANES : (t + 1) * LANES]

    def finish(jl, slot):
        for k in range(k_len):
            g = g_s[slot, pl.ds(k, ci, stride=row), :]
            o_ref[jl, k] = (v_ref[jl, k].astype(F32) + g).astype(BF16)

    def body(step, _):
        for q in range(ZQ):
            mixer.filt(step * ZQ + q, q)
        for q in range(ZQ):
            mix(q)
            if q:
                finish(step * ZQ + q - 1, q - 1)
        finish(step * ZQ + ZQ - 1, ZQ - 1)
        return 0

    lax.fori_loop(0, mixer.jb // ZQ, body, 0)


def z_mix(mats, w4, bias, layer, u2, nb, vol, half):

    ci, jl_len, k_len, _ = u2.shape
    size = jl_len * k_len * ci * LANES
    vol_spec = pl.BlockSpec((8, k_len, ci, LANES), lambda s: (s, 0, 0, 0))
    return pl.pallas_call(
        functools.partial(z_kernel, half),
        grid=(jl_len // 8,),
        in_specs=[
            pl.BlockSpec((1, *mats.shape[1:]), lambda s: (layer, 0, 0)),
            pl.BlockSpec((1, *w4.shape[1:]), lambda s: (layer, 0, 0)),
            pl.BlockSpec((1, *bias.shape[1:]), lambda s: (layer, 0, 0)),
            pl.BlockSpec((ci, 8, k_len, LANES), lambda s: (0, s, 0, 0)),
            pl.BlockSpec((ci, 1, half, 8, LANES), lambda s: (0, s, 0, 0, 0)),
            vol_spec,
        ],
        out_specs=vol_spec,
        scratch_shapes=[
            pltpu.VMEM((ci * 16 * (8 + PAD), LANES), F32),
            pltpu.VMEM((ZQ, ci // 2 * k_len, 2 * LANES), BF16),
            pltpu.VMEM((ZQ, ci * (k_len + PAD), LANES), F32),
        ],
        out_shape=jax.ShapeDtypeStruct(vol.shape, BF16),
        cost_estimate=pl.CostEstimate(flops=size * 160 * 6, bytes_accessed=size * 7, transcendentals=size),
        name="z_mix",
    )(mats, w4, bias, u2, nb, vol)


def enter_kernel(meta, eye_ref, lo_ref, hi_ref, o_ref, s_ref, t_ref):
    chans, ci, jb, k_len = lo_ref.shape
    eye = eye_ref[...]
    pitch, row = jb + PAD, k_len + PAD

    def spread(c, _):
        for h, ref in enumerate((lo_ref, hi_ref)):
            for ip in range(ci // 2):
                rows = pl.ds(((ip * 2 + h) * chans + c) * pitch, jb)
                s_ref[rows, :] = jnp.concatenate([ref[c, 2 * ip].astype(F32), ref[c, 2 * ip + 1].astype(F32)], axis=1)
        return 0

    lax.fori_loop(0, chans, spread, 0, unroll=16)

    def turn(jl, slot):
        for ip in range(0, ci // 2, 2):
            parts = [
                s_ref[pl.ds((ip + u) * 2 * chans * pitch + jl, 2 * chans, stride=pitch), :].astype(BF16) for u in range(2)
            ]
            out = lax.dot_general(eye, jnp.concatenate(parts, axis=0), NT, preferred_element_type=F32)
            for u in range(2):
                for t in range(2):
                    done = out[t * k_len : (t + 1) * k_len, u * LANES : (u + 1) * LANES]
                    t_ref[slot, pl.ds((2 * (ip + u) + t) * row, k_len), :] = done

    def finish(jl, slot):
        for k in range(k_len):
            o_ref[jl, k] = t_ref[slot, pl.ds(k, ci, stride=row), :].astype(BF16)

    def body(step, _):
        for q in range(EQ):
            turn(EQ * step + q, q)
            if q:
                finish(EQ * step + q - 1, q - 1)
        finish(EQ * step + EQ - 1, EQ - 1)
        return 0

    lax.fori_loop(0, jb // EQ, body, 0)


def enter(meta, volume, p, n_chunks):
    chans, _, j_len, k_len = volume.shape
    jl_len, jb = j_len // 2, EJ

    def spot(h):
        return lambda s, m: (0, jnp.where(m[0] == 0, p, n_chunks - 1 - p), s + h * (jl_len // jb), 0)

    blocks = [pl.BlockSpec((chans, CI, jb, k_len), spot(h)) for h in range(2)]
    size = chans * CI * j_len * k_len
    return pl.pallas_call(
        enter_kernel,
        grid_spec=pltpu.PrefetchScalarGridSpec(
            num_scalar_prefetch=1,
            grid=(jl_len // jb,),
            in_specs=[pl.BlockSpec((2 * k_len, 2 * k_len), lambda s, m: (0, 0))] + blocks,
            out_specs=pl.BlockSpec((jb, k_len, CI, 2 * chans), lambda s, m: (s, 0, 0, 0)),
            scratch_shapes=[
                pltpu.VMEM((CI * chans * (jb + PAD), 2 * k_len), F32),
                pltpu.VMEM((EQ, CI * (k_len + PAD), 2 * chans), F32),
            ],
        ),
        out_shape=jax.ShapeDtypeStruct((jl_len, k_len, CI, 2 * chans), BF16),
        cost_estimate=pl.CostEstimate(flops=size * 512, bytes_accessed=size * 6, transcendentals=0),
        name="enter",
    )(meta, jnp.eye(2 * k_len, dtype=BF16), volume, volume)


def leave_kernel(meta, eye_ref, v_ref, *refs):
    o_ref, t_ref, s_ref = refs[-3:]
    jb, k_len, ci, lanes = v_ref.shape
    chans = lanes // 2
    h = pl.program_id(1)
    pitch, row = jb + PAD, ci + PAD
    eye = eye_ref[...]

    @pl.when(h == 0)
    def _():
        def spread(jl, slot):
            for k in range(k_len):
                t_ref[slot, pl.ds(k * row, ci), :] = v_ref[jl, k].astype(F32)

        def turn(jl, slot):
            for ip in range(0, ci // 2, 2):
                parts = [t_ref[slot, pl.ds(2 * ip + t, k_len, stride=row), :].astype(BF16) for t in range(4)]
                out = lax.dot_general(eye, jnp.concatenate(parts, axis=0), NT, preferred_element_type=F32)
                for u in range(2):
                    rows = pl.ds((ip + u) * lanes * pitch + jl, lanes, stride=pitch)
                    s_ref[rows, :] = out[:, u * LANES : (u + 1) * LANES]

        def body(step, _):
            for q in range(LQ):
                spread(LQ * step + q, q)
                if q:
                    turn(LQ * step + q - 1, q - 1)
            turn(LQ * step + LQ - 1, LQ - 1)
            return 0

        lax.fori_loop(0, jb // LQ, body, 0)

    def pack(c, _):
        for ip in range(ci // 2):
            both = s_ref[pl.ds((ip * lanes + h * chans + c) * pitch, jb), :]
            o_ref[c, 2 * ip] = both[:, :k_len].astype(BF16)
            o_ref[c, 2 * ip + 1] = swap_halves(both)[:, :k_len].astype(BF16)
        return 0

    lax.fori_loop(0, chans, pack, 0, unroll=16)


def leave(meta, vol, out, p, n_chunks):
    jl_len, k_len, ci, lanes = vol.shape
    chans, jb = lanes // 2, LJ
    j_len = 2 * jl_len

    def spot(s, h, m):
        return (0, jnp.where(m[0] == 0, p, n_chunks - 1 - p), s + h * (jl_len // jb), 0)

    size = chans * CI * j_len * k_len
    more = [] if out is None else [out]
    return pl.pallas_call(
        leave_kernel,
        grid_spec=pltpu.PrefetchScalarGridSpec(
            num_scalar_prefetch=1,
            grid=(jl_len // jb, 2),
            in_specs=[
                pl.BlockSpec((lanes, lanes), lambda s, h, m: (0, 0)),
                pl.BlockSpec((jb, k_len, ci, lanes), lambda s, h, m: (s, 0, 0, 0)),
            ]
            + [pl.BlockSpec(memory_space=pl.ANY) for _ in more],
            out_specs=pl.BlockSpec((chans, CI, jb, k_len), spot),
            scratch_shapes=[
                pltpu.VMEM((LQ, k_len * (ci + PAD), lanes), F32),
                pltpu.VMEM((CI // 2 * lanes * (jb + PAD), 2 * k_len), F32),
            ],
        ),
        out_shape=jax.ShapeDtypeStruct((chans, n_chunks * CI, j_len, k_len), BF16),
        input_output_aliases={3: 0} if more else {},
        cost_estimate=pl.CostEstimate(flops=size * 512, bytes_accessed=size * 6, transcendentals=0),
        name="leave",
    )(meta, jnp.eye(lanes, dtype=BF16), vol, *more)


SWAP = [(0, 1), (1, 0)]
ORDER = (
    "e3", "e2", "e1", "x031", "e0", "x021", "y03", "x002", "y02", "z03",
    "y00", "z02", "y01", "x131", "z00", "z01", "x101", "y13", "x112", "y10",
    "z13", "y11", "z10", "y12", "z11", "x201", "z12", "x231", "y20", "x212",
    "y23", "z20", "l0", "y21", "y22", "z23", "l3", "z21", "z22", "l2",
    "l1",
)


def solution(mesh):
    def local_layers(volume, filter_taps, mix_w, mix_bias):
        _, i_len, j_len, k_len = volume.shape
        layers = filter_taps.shape[0]
        half = (filter_taps.shape[2] - 1) // 2
        jl_len, n_chunks = j_len // 2, i_len // CI
        x_pos, y_pos, z_pos = (lax.axis_index(a) for a in ("x", "y", "z"))
        meta = jnp.stack([x_pos, y_pos, z_pos]).astype(jnp.int32)
        mats_x = band_x(filter_taps[:, 0], x_pos)
        mats_y = band_y(filter_taps[:, 1], y_pos, jl_len)
        mats_z = band_z(filter_taps[:, 2], z_pos, k_len)
        w4 = jax.vmap(lambda w: jnp.kron(jnp.eye(4, dtype=BF16), w))(mix_w)
        bias = jnp.tile(mix_bias, (1, 4))[:, None, :]

        vols, u2, far_y, far_z, beyond = {}, {}, {}, {}, {}
        out = None

        def settle(layer, p, vol):
            vols[layer, p] = vol
            if p == n_chunks - 1 and layer < layers:
                beyond[layer] = lax.ppermute(vol, "x", SWAP)

        for op in ORDER:
            kind, p = op[0], int(op[1] if op[0] in "el" else op[2])
            layer = int(op[1])
            if kind == "e":
                settle(0, p, enter(meta, volume, p, n_chunks))
            elif kind == "x":
                n_own = int(op[3])
                own = [vols[layer, q] for q in range(max(p - 1, 0), p + n_own)]
                after = vols[layer, p + n_own] if p + n_own < n_chunks else beyond[layer]
                first = 0 if p else CI
                mats = mats_x[:, : n_own * CI, first : (n_own + 2) * CI]
                u1, *send = x_pass(meta, mats, layer, own + [after], half)
                for t in range(n_own):
                    far_y[p + t] = (u1, t, lax.ppermute(send[t], "y", SWAP))
            elif kind == "y":
                u2[p], send = y_pass(meta, mats_y, layer, *far_y[p], half)
                far_z[p] = lax.ppermute(send, "z", SWAP)
            elif kind == "z":
                settle(layer + 1, p, z_mix(mats_z, w4, bias, layer, u2[p], far_z[p], vols[layer, p], half))
            else:
                out = leave(meta, vols[layers, p], out, p, n_chunks)
        return out

    vol_spec = P("batch", "x", "y", "z")
    return jax.shard_map(local_layers, mesh=mesh, in_specs=(vol_spec, P(), P(), P()), out_specs=vol_spec, check_vma=False)
```

```python
import functools

import jax
import jax.numpy as jnp
from jax import lax
from jax.experimental import pallas as pl
from jax.experimental.pallas import tpu as pltpu
from jax.sharding import PartitionSpec as P


CI = 16
NT = (((1,), (1,)), ((), ()))
KB = 16
XQ = 4
YI = 4
YQ = 4
ZQ = 4
LJ = 16
LQ = 4
EJ = 16
EQ = 4
VMEM_BYTES = 67_043_328
PAD = 1
LANES = 128
F32 = jnp.float32
BF16 = jnp.bfloat16


def toeplitz(taps, offset):
    half = (taps.shape[1] - 1) // 2
    hits = (offset + half)[None, ..., None] == jnp.arange(taps.shape[1])
    taps_b = taps.astype(BF16).astype(F32)
    return jnp.sum(jnp.where(hits, taps_b[:, None, None, :], 0.0), axis=-1).astype(BF16)


def band_x(taps, x_pos):
    n = jnp.arange(2 * CI)[:, None]
    q = jnp.arange(4 * CI)[None, :]
    sign = jnp.where(x_pos == 0, 1, -1)
    return toeplitz(taps, sign * CI * (q // CI - 1 - n // CI) + q % CI - n % CI)


FAR = 10**6


def band_y(taps, y_pos, jl_len):
    half = (taps.shape[1] - 1) // 2
    n = jnp.arange(jl_len)[:, None]
    m = jnp.arange(jl_len)
    r = jnp.arange(16)
    other = jnp.where(m < jl_len // 2, m + jl_len, m - jl_len)
    beyond = jnp.where(r < half, jnp.where(y_pos == 0, jl_len + r, r - half), FAR)
    return toeplitz(taps, jnp.concatenate([m, other, beyond])[None, :] - n)


def band_z(taps, z_pos, k_len):
    half = (taps.shape[1] - 1) // 2
    n = jnp.arange(k_len)[:, None]
    r = jnp.arange(16)
    beyond = jnp.where(r < half, jnp.where(z_pos == 0, k_len + r, r - half), FAR)
    return toeplitz(taps, jnp.concatenate([jnp.arange(k_len), beyond])[None, :] - n)


def lane_low(shape):
    return lax.broadcasted_iota(jnp.int32, shape, 1) < LANES // 2


def swap_halves(v):
    return pltpu.roll(v, LANES // 2, 1)


def x_kernel(n_in, first_in, half, meta, a_ref, *refs):
    vols, u_ref, sends, s_ref = refs[:n_in], refs[n_in], refs[n_in + 1 : -1], refs[-1]
    jl_len, ci = vols[0].shape[0], vols[0].shape[2]
    planes = len(sends) * ci
    row = planes + PAD
    y_pos = meta[1]
    first = jnp.where(y_pos == 0, jl_len - half, 0)
    group = 8
    mat = a_ref[0][:planes, first_in * ci : (first_in + n_in) * ci]

    def pair(kp, slot):
        for par in range(2):
            k = kp * 2 + par
            for g in range(0, jl_len, group):
                rhs = jnp.concatenate(
                    [jnp.concatenate([v[jl, k] for v in vols], axis=0) for jl in range(g, g + group)], axis=1
                )
                out = jnp.dot(mat, rhs, preferred_element_type=F32)
                for t in range(group):
                    s_ref[slot + par, pl.ds((g + t) * row, planes), :] = out[:, t * LANES : (t + 1) * LANES]

    def finish(kp, slot):
        for par in range(2):
            for i in range(planes):
                u_ref[i, kp * 2 + par] = s_ref[slot + par, pl.ds(i, jl_len, stride=row), :].astype(BF16)
        for r in range(half):
            for part, send_ref in enumerate(sends):
                rows = pl.ds((first + r) * row + part * ci, ci)
                even, odd = s_ref[slot, rows, :], s_ref[slot + 1, rows, :]
                low = lane_low(even.shape)
                up = jnp.where(low, swap_halves(even), odd)
                down = jnp.where(low, even, swap_halves(odd))
                send_ref[kp, r] = jnp.where(y_pos == 0, up, down).astype(BF16)

    def body(step, _):
        for q in range(XQ):
            pair(step * XQ + q, 2 * q)
            if q:
                finish(step * XQ + q - 1, 2 * (q - 1))
        finish(step * XQ + XQ - 1, 2 * (XQ - 1))
        return 0

    lax.fori_loop(0, vols[0].shape[1] // (2 * XQ), body, 0)


def x_pass(meta, mats, layer, vols, n_own, half):
    jl_len, k_len, ci, _ = vols[0].shape
    n_in = len(vols)
    vol_spec = pl.BlockSpec((jl_len, KB, ci, LANES), lambda s, m: (0, s, 0, 0))
    send_spec = pl.BlockSpec((KB // 2, half, ci, LANES), lambda s, m: (s, 0, 0, 0))
    send_shape = jax.ShapeDtypeStruct((k_len // 2, half, ci, LANES), BF16)
    size = jl_len * k_len * ci * LANES
    return pl.pallas_call(
        functools.partial(x_kernel, n_in, n_own + 2 - n_in, half),
        grid_spec=pltpu.PrefetchScalarGridSpec(
            num_scalar_prefetch=1,
            grid=(k_len // KB,),
            in_specs=[pl.BlockSpec((1, *mats.shape[1:]), lambda s, m: (layer, 0, 0))] + [vol_spec] * n_in,
            out_specs=[pl.BlockSpec((n_own * ci, KB, jl_len, LANES), lambda s, m: (0, s, 0, 0))] + [send_spec] * n_own,
            scratch_shapes=[pltpu.VMEM((2 * XQ, jl_len * (n_own * ci + PAD), LANES), F32)],
        ),
        out_shape=[jax.ShapeDtypeStruct((n_own * ci, k_len, jl_len, LANES), BF16)] + [send_shape] * n_own,
        cost_estimate=pl.CostEstimate(flops=size * 512 * n_own, bytes_accessed=size * 2 * (n_in + n_own), transcendentals=0),
        name="x_pass",
    )(meta, mats, *vols)


def y_kernel(half, meta, a_ref, u_ref, nb_ref, o_ref, send_ref, nb_s, s_ref):
    y_pos, z_pos = meta[1], meta[2]
    k_len, jl_len = u_ref.shape[1], u_ref.shape[2]
    ci = nb_ref.shape[2]
    mat = a_ref[0]
    pitch = ci + PAD
    span = 16 * pitch
    row = jl_len + PAD

    @pl.when(pl.program_id(0) == 0)
    def _():
        def fill(kp, _):
            for r in range(16):
                rows = pl.ds(kp * span + r * pitch, ci)
                nb_s[rows, :] = nb_ref[kp, r].astype(F32) if r < half else jnp.zeros((ci, LANES), F32)
            return 0

        lax.fori_loop(0, k_len // 2, fill, 0)

    first = jnp.where(z_pos == 0, k_len - half, 0)

    def quad(here_i, slot, kq):
        i = pl.program_id(0) * YI + here_i
        parts = []
        for pr in range(2):
            kp = kq * 2 + pr
            nb = nb_s[pl.ds(kp * span + i, 16, stride=pitch), :]
            turned = swap_halves(nb)
            here = lane_low(nb.shape) == (y_pos != 0)
            for par in range(2):
                k = kp * 2 + par
                own = u_ref[here_i, k]
                other = swap_halves(own.astype(F32))
                top = lax.broadcasted_iota(jnp.int32, other.shape, 0) < jl_len // 2
                other = jnp.where(top == lane_low(other.shape), other, 0.0).astype(BF16)
                stay = (y_pos == 0) if par else (y_pos != 0)
                far = jnp.where(here, jnp.where(stay, nb, turned), 0.0).astype(BF16)
                parts.append(jnp.concatenate([own, other, far], axis=0))
        out = jnp.dot(mat, jnp.concatenate(parts, axis=1), preferred_element_type=F32)
        for t in range(4):
            rows = pl.ds((kq * 4 + t) * row, jl_len)
            s_ref[slot, rows, :] = out[:, t * LANES : (t + 1) * LANES]

    def finish(here_i, slot):
        for jl in range(jl_len):
            o_ref[here_i, jl] = s_ref[slot, pl.ds(jl, k_len, stride=row), :].astype(BF16)
        for r in range(half):
            for jb in range(jl_len // 8):
                rows = pl.ds((first + r) * row + jb * 8, 8)
                send_ref[here_i, jb, r] = s_ref[slot, rows, :].astype(BF16)

    def body(step, _):
        for q in range(YQ):
            for kq in range(k_len // 4):
                quad(step * YQ + q, q, kq)
            if q:
                finish(step * YQ + q - 1, q - 1)
        finish(step * YQ + YQ - 1, YQ - 1)
        return 0

    lax.fori_loop(0, YI // YQ, body, 0)


def y_pass(meta, mats, layer, u1, part, nb, half):

    ci, k_len, jl_len = nb.shape[2], u1.shape[1], u1.shape[2]
    size = jl_len * k_len * ci * LANES
    return pl.pallas_call(
        functools.partial(y_kernel, half),
        grid_spec=pltpu.PrefetchScalarGridSpec(
            num_scalar_prefetch=1,
            grid=(ci // YI,),
            in_specs=[
                pl.BlockSpec((1, *mats.shape[1:]), lambda s, m: (layer, 0, 0)),
                pl.BlockSpec((YI, k_len, jl_len, LANES), lambda s, m: (s + part * (ci // YI), 0, 0, 0)),
                pl.BlockSpec(nb.shape, lambda s, m: (0, 0, 0, 0)),
            ],
            out_specs=[
                pl.BlockSpec((YI, jl_len, k_len, LANES), lambda s, m: (s, 0, 0, 0)),
                pl.BlockSpec((YI, jl_len // 8, half, 8, LANES), lambda s, m: (s, 0, 0, 0, 0)),
            ],
            scratch_shapes=[
                pltpu.VMEM((k_len // 2 * 16 * (ci + PAD), LANES), F32),
                pltpu.VMEM((YQ, k_len * (jl_len + PAD), LANES), F32),
            ],
        ),
        out_shape=[
            jax.ShapeDtypeStruct((ci, jl_len, k_len, LANES), BF16),
            jax.ShapeDtypeStruct((ci, jl_len // 8, half, 8, LANES), BF16),
        ],
        cost_estimate=pl.CostEstimate(flops=size * 160 * 4, bytes_accessed=size * 5, transcendentals=0),
        compiler_params=pltpu.CompilerParams(vmem_limit_bytes=VMEM_BYTES),
        name="y_pass",
    )(meta, mats, u1, nb)


class Mixer:
    def __init__(self, half, a_ref, w_ref, b_ref, u_ref, nb_ref, nb_s):
        self.ci, self.jb, self.k_len = u_ref.shape[0], u_ref.shape[1], u_ref.shape[2]
        self.half, self.a_ref, self.w_ref, self.b_ref = half, a_ref, w_ref, b_ref
        self.u_ref, self.nb_ref, self.nb_s = u_ref, nb_ref, nb_s
        self.pitch = self.jb + PAD
        self.span = 16 * self.pitch

    def fill(self):
        def one(i, _):
            for r in range(16):
                rows = pl.ds(i * self.span + r * self.pitch, self.jb)
                far = self.nb_ref[i, 0, r].astype(F32) if r < self.half else jnp.zeros((self.jb, LANES), F32)
                self.nb_s[rows, :] = far
            return 0

        lax.fori_loop(0, self.ci, one, 0)

    def gelu(self, jl, ip0):
        rows = []
        for ip in (ip0, ip0 + 1):
            parts = []
            for i in (2 * ip, 2 * ip + 1):
                far = self.nb_s[pl.ds(i * self.span + jl, 16, stride=self.pitch), :].astype(BF16)
                parts.append(jnp.concatenate([self.u_ref[i, jl], far], axis=0))
            u3 = jnp.dot(self.a_ref[0], jnp.concatenate(parts, axis=1), preferred_element_type=F32)
            rows.append(u3.astype(BF16))
        m = jnp.dot(jnp.concatenate(rows, axis=0), self.w_ref[0], preferred_element_type=F32) + self.b_ref[0]
        return 0.5 * m * (1.0 + lax.erf(m * 0.7071067811865476))


def z_kernel(half, a_ref, w_ref, b_ref, u_ref, nb_ref, v_ref, o_ref, nb_s, g_s):
    mixer = Mixer(half, a_ref, w_ref, b_ref, u_ref, nb_ref, nb_s)
    ci, k_len = mixer.ci, mixer.k_len
    row = k_len + PAD
    mixer.fill()

    def mix(jl, slot):
        for ip in range(0, ci // 2, 2):
            g = mixer.gelu(jl, ip)
            for i in range(4):
                part = g[i // 2 * k_len : (i // 2 + 1) * k_len, i % 2 * LANES : (i % 2 + 1) * LANES]
                g_s[slot, pl.ds((2 * ip + i) * row, k_len), :] = part

    def finish(jl, slot):
        for k in range(k_len):
            g = g_s[slot, pl.ds(k, ci, stride=row), :]
            o_ref[jl, k] = (v_ref[jl, k].astype(F32) + g).astype(BF16)

    def body(step, _):
        for q in range(ZQ):
            mix(step * ZQ + q, q)
            if q:
                finish(step * ZQ + q - 1, q - 1)
        finish(step * ZQ + ZQ - 1, ZQ - 1)
        return 0

    lax.fori_loop(0, mixer.jb // ZQ, body, 0)


def z_mix(mats, w4, bias, layer, u2, nb, vol, half):

    ci, jl_len, k_len, _ = u2.shape
    size = jl_len * k_len * ci * LANES
    vol_spec = pl.BlockSpec((8, k_len, ci, LANES), lambda s: (s, 0, 0, 0))
    return pl.pallas_call(
        functools.partial(z_kernel, half),
        grid=(jl_len // 8,),
        in_specs=[
            pl.BlockSpec((1, *mats.shape[1:]), lambda s: (layer, 0, 0)),
            pl.BlockSpec((1, *w4.shape[1:]), lambda s: (layer, 0, 0)),
            pl.BlockSpec((1, *bias.shape[1:]), lambda s: (layer, 0, 0)),
            pl.BlockSpec((ci, 8, k_len, LANES), lambda s: (0, s, 0, 0)),
            pl.BlockSpec((ci, 1, half, 8, LANES), lambda s: (0, s, 0, 0, 0)),
            vol_spec,
        ],
        out_specs=vol_spec,
        scratch_shapes=[
            pltpu.VMEM((ci * 16 * (8 + PAD), LANES), F32),
            pltpu.VMEM((ZQ, ci * (k_len + PAD), LANES), F32),
        ],
        out_shape=jax.ShapeDtypeStruct(vol.shape, BF16),
        cost_estimate=pl.CostEstimate(flops=size * 160 * 6, bytes_accessed=size * 7, transcendentals=size),
        compiler_params=pltpu.CompilerParams(vmem_limit_bytes=VMEM_BYTES),
        name="z_mix",
    )(mats, w4, bias, u2, nb, vol)


def enter_kernel(meta, eye_ref, lo_ref, hi_ref, o_ref, s_ref, t_ref):
    chans, ci, jb, k_len = lo_ref.shape
    eye = eye_ref[...]
    pitch, row = jb + PAD, k_len + PAD

    def spread(c, _):
        for h, ref in enumerate((lo_ref, hi_ref)):
            for ip in range(ci // 2):
                rows = pl.ds(((ip * 2 + h) * chans + c) * pitch, jb)
                s_ref[rows, :] = jnp.concatenate([ref[c, 2 * ip].astype(F32), ref[c, 2 * ip + 1].astype(F32)], axis=1)
        return 0

    lax.fori_loop(0, chans, spread, 0, unroll=16)

    def turn(jl, slot):
        for ip in range(0, ci // 2, 2):
            parts = [
                s_ref[pl.ds((ip + u) * 2 * chans * pitch + jl, 2 * chans, stride=pitch), :].astype(BF16) for u in range(2)
            ]
            out = lax.dot_general(eye, jnp.concatenate(parts, axis=0), NT, preferred_element_type=F32)
            for u in range(2):
                for t in range(2):
                    done = out[t * k_len : (t + 1) * k_len, u * LANES : (u + 1) * LANES]
                    t_ref[slot, pl.ds((2 * (ip + u) + t) * row, k_len), :] = done

    def finish(jl, slot):
        for k in range(k_len):
            o_ref[jl, k] = t_ref[slot, pl.ds(k, ci, stride=row), :].astype(BF16)

    def body(step, _):
        for q in range(EQ):
            turn(EQ * step + q, q)
            if q:
                finish(EQ * step + q - 1, q - 1)
        finish(EQ * step + EQ - 1, EQ - 1)
        return 0

    lax.fori_loop(0, jb // EQ, body, 0)


def enter(meta, volume, p, n_chunks):
    chans, _, j_len, k_len = volume.shape
    jl_len, jb = j_len // 2, EJ

    def spot(h):
        return lambda s, m: (0, jnp.where(m[0] == 0, p, n_chunks - 1 - p), s + h * (jl_len // jb), 0)

    blocks = [pl.BlockSpec((chans, CI, jb, k_len), spot(h)) for h in range(2)]
    size = chans * CI * j_len * k_len
    return pl.pallas_call(
        enter_kernel,
        grid_spec=pltpu.PrefetchScalarGridSpec(
            num_scalar_prefetch=1,
            grid=(jl_len // jb,),
            in_specs=[pl.BlockSpec((2 * k_len, 2 * k_len), lambda s, m: (0, 0))] + blocks,
            out_specs=pl.BlockSpec((jb, k_len, CI, 2 * chans), lambda s, m: (s, 0, 0, 0)),
            scratch_shapes=[
                pltpu.VMEM((CI * chans * (jb + PAD), 2 * k_len), F32),
                pltpu.VMEM((EQ, CI * (k_len + PAD), 2 * chans), F32),
            ],
        ),
        out_shape=jax.ShapeDtypeStruct((jl_len, k_len, CI, 2 * chans), BF16),
        cost_estimate=pl.CostEstimate(flops=size * 512, bytes_accessed=size * 6, transcendentals=0),
        name="enter",
    )(meta, jnp.eye(2 * k_len, dtype=BF16), volume, volume)


def leave_kernel(meta, eye_ref, v_ref, *refs):
    o_ref, t_ref, s_ref = refs[-3:]
    jb, k_len, ci, lanes = v_ref.shape
    chans = lanes // 2
    h = pl.program_id(1)
    pitch, row = jb + PAD, ci + PAD
    eye = eye_ref[...]

    @pl.when(h == 0)
    def _():
        def spread(jl, slot):
            for k in range(k_len):
                t_ref[slot, pl.ds(k * row, ci), :] = v_ref[jl, k].astype(F32)

        def turn(jl, slot):
            for ip in range(0, ci // 2, 2):
                parts = [t_ref[slot, pl.ds(2 * ip + t, k_len, stride=row), :].astype(BF16) for t in range(4)]
                out = lax.dot_general(eye, jnp.concatenate(parts, axis=0), NT, preferred_element_type=F32)
                for u in range(2):
                    rows = pl.ds((ip + u) * lanes * pitch + jl, lanes, stride=pitch)
                    s_ref[rows, :] = out[:, u * LANES : (u + 1) * LANES]

        def body(step, _):
            for q in range(LQ):
                spread(LQ * step + q, q)
                if q:
                    turn(LQ * step + q - 1, q - 1)
            turn(LQ * step + LQ - 1, LQ - 1)
            return 0

        lax.fori_loop(0, jb // LQ, body, 0)

    def pack(c, _):
        for ip in range(ci // 2):
            both = s_ref[pl.ds((ip * lanes + h * chans + c) * pitch, jb), :]
            o_ref[c, 2 * ip] = both[:, :k_len].astype(BF16)
            o_ref[c, 2 * ip + 1] = swap_halves(both)[:, :k_len].astype(BF16)
        return 0

    lax.fori_loop(0, chans, pack, 0, unroll=16)


def leave(meta, vol, out, p, n_chunks):
    jl_len, k_len, ci, lanes = vol.shape
    chans, jb = lanes // 2, LJ
    j_len = 2 * jl_len

    def spot(s, h, m):
        return (0, jnp.where(m[0] == 0, p, n_chunks - 1 - p), s + h * (jl_len // jb), 0)

    size = chans * CI * j_len * k_len
    more = [] if out is None else [out]
    return pl.pallas_call(
        leave_kernel,
        grid_spec=pltpu.PrefetchScalarGridSpec(
            num_scalar_prefetch=1,
            grid=(jl_len // jb, 2),
            in_specs=[
                pl.BlockSpec((lanes, lanes), lambda s, h, m: (0, 0)),
                pl.BlockSpec((jb, k_len, ci, lanes), lambda s, h, m: (s, 0, 0, 0)),
            ]
            + [pl.BlockSpec(memory_space=pl.ANY) for _ in more],
            out_specs=pl.BlockSpec((chans, CI, jb, k_len), spot),
            scratch_shapes=[
                pltpu.VMEM((LQ, k_len * (ci + PAD), lanes), F32),
                pltpu.VMEM((CI // 2 * lanes * (jb + PAD), 2 * k_len), F32),
            ],
        ),
        out_shape=jax.ShapeDtypeStruct((chans, n_chunks * CI, j_len, k_len), BF16),
        input_output_aliases={3: 0} if more else {},
        cost_estimate=pl.CostEstimate(flops=size * 512, bytes_accessed=size * 6, transcendentals=0),
        name="leave",
    )(meta, jnp.eye(lanes, dtype=BF16), vol, *more)


SWAP = [(0, 1), (1, 0)]
ORDER = (
    "e2", "e1", "e3", "x021", "x031", "e0", "y02", "x002", "y03", "z02",
    "y00", "z03", "y01", "z00", "x131", "z01", "x102", "y13", "x121", "y10",
    "z13", "y11", "z10", "y12", "z11", "x201", "z12", "x211", "y20", "x222",
    "y21", "z20", "l0", "y22", "z21", "y23", "l1", "z22", "z23", "l3",
    "l2",
)


def solution(mesh):
    def local_layers(volume, filter_taps, mix_w, mix_bias):
        _, i_len, j_len, k_len = volume.shape
        layers = filter_taps.shape[0]
        half = (filter_taps.shape[2] - 1) // 2
        jl_len, n_chunks = j_len // 2, i_len // CI
        x_pos, y_pos, z_pos = (lax.axis_index(a) for a in ("x", "y", "z"))
        meta = jnp.stack([x_pos, y_pos, z_pos]).astype(jnp.int32)
        mats_x = band_x(filter_taps[:, 0], x_pos)
        mats_y = band_y(filter_taps[:, 1], y_pos, jl_len)
        mats_z = band_z(filter_taps[:, 2], z_pos, k_len)
        w4 = jax.vmap(lambda w: jnp.kron(jnp.eye(4, dtype=BF16), w))(mix_w)
        bias = jnp.tile(mix_bias, (1, 4))[:, None, :]

        vols, u2, far_y, far_z, beyond = {}, {}, {}, {}, {}
        out = None

        def settle(layer, p, vol):
            vols[layer, p] = vol
            if p == n_chunks - 1 and layer < layers:
                beyond[layer] = lax.ppermute(vol, "x", SWAP)

        for op in ORDER:
            kind, p = op[0], int(op[1] if op[0] in "el" else op[2])
            layer = int(op[1])
            if kind == "e":
                settle(0, p, enter(meta, volume, p, n_chunks))
            elif kind == "x":
                n_own = int(op[3])
                own = [vols[layer, q] for q in range(max(p - 1, 0), p + n_own)]
                after = vols[layer, p + n_own] if p + n_own < n_chunks else beyond[layer]
                u1, *send = x_pass(meta, mats_x, layer, own + [after], n_own, half)
                for t in range(n_own):
                    far_y[p + t] = (u1, t, lax.ppermute(send[t], "y", SWAP))
            elif kind == "y":
                u2[p], send = y_pass(meta, mats_y, layer, *far_y[p], half)
                far_z[p] = lax.ppermute(send, "z", SWAP)
            elif kind == "z":
                settle(layer + 1, p, z_mix(mats_z, w4, bias, layer, u2[p], far_z[p], vols[layer, p], half))
            else:
                out = leave(meta, vols[layers, p], out, p, n_chunks)
        return out

    vol_spec = P("batch", "x", "y", "z")
    return jax.shard_map(local_layers, mesh=mesh, in_specs=(vol_spec, P(), P(), P()), out_specs=vol_spec, check_vma=False)
```
